512 devices in a mesh: sp: 64 (over y, x, core), pb: 8 (over z).
Axes of the slice: x: 4, y: 8, z: 8, core: 2. Of those that a mesh axis runs over, the one named last changes fastest.
Arguments:
- amplitudes: bfloat16 [160, 1024, 1024], P('pb', 'sp'), may hold values from -6 to 6
- virtuals: bfloat16 [1400, 1024], replicated, may hold values from -0.375 to 0.375
- energies: float32 [1024], replicated, may hold values from 0.02 to 0.2
- integrals: bfloat16 [8192, 2048], P('sp'), may hold values from -0.125 to 0.125
- screened: int32 [64, 16], P('sp'), may hold values from 0 to 63, as said below
- counts: int32 [64], P('sp'), may hold values from 1 to 16, 512 in all
- offsets: int32 [2, 64], replicated, may hold values from 0 to 1384
- coupling: bfloat16 [160, 160], P('pb'), may hold values from -0.5 to 0.5
Outputs:
- residual: bfloat16 [160, 1024, 1024], P('pb', 'sp')
The draws below stay inside these ranges and needn't reach their ends.
Inputs may be any that keep to these rules, and one draw needn't show every extreme that they name: `screened`: each row names 16 different blocks.
All inputs are finite; a program needn't handle non-finite values. No bound on the sum of `counts` on one device may be relied on, other than what follows from the above.
Results may differ from the reference program's by a relative error of at most 0.01.
Values may be sent and summed in bfloat16 or wider, within the bound.
A program may use at most 64 MiB of HBM per device.

```python
import math
import jax
import jax.numpy as jnp
import numpy as np
from jax import lax

NAO = 1400
NEXT = 1024
SHELL_ROW = 8
SHELL_COL = 16
KSCR = 16
NPAIR = 160
NBLK = 64


def draw_screened(key, part):
    keys = jax.random.split(jax.random.fold_in(key, 7), NBLK)
    rows = jax.vmap(lambda single: jax.random.permutation(single, NBLK)[:KSCR])(keys)
    return rows.astype(jnp.int32)


def set_ends(drawn, key, smallest, top_value):
    dims = drawn.shape
    index_at = [jax.random.randint(jax.random.fold_in(key, axis), (), 0, dims[axis]) for axis in range(len(dims))]
    drawn = drawn.at[tuple(index_at)].set(smallest)
    longest = dims.index(max(dims))
    index_at[longest] = (index_at[longest] + 1) % dims[longest]
    return drawn.at[tuple(index_at)].set(top_value)


def steps_of(own_key, dims, pieces, low, largest):
    gain, own = 1.0, jax.random.fold_in(own_key, 6)
    for axis_at, shards_of in pieces:
        heights = jnp.exp(jax.random.uniform(jax.random.fold_in(own, axis_at), (shards_of,), jnp.float32, low / len(pieces), largest / len(pieces)))
        gain = gain * jnp.repeat(heights, dims[axis_at] // shards_of).reshape([-1 if axis == axis_at else 1 for axis in range(len(dims))])
    return gain


def length_profile(count, total, reach, lean):
    weights = [(1 << 20) // math.isqrt(rank ** lean) + 1 for rank in range(2, count + 1)]
    spare, given = total - reach - (count - 1), [1] * (count - 1)
    while spare > 0:
        candidates = [i for i in range(count - 1) if given[i] < reach]
        mass, left = sum([weights[i] for i in candidates]), spare
        for i in candidates:
            addition = min(reach - given[i], max(1, left * weights[i] // mass), spare)
            given[i] = given[i] + addition
            spare = spare - addition
    return np.array([reach] + given)


def ragged_sizes(rng, amount, total, bound, skew):
    if amount == 2:
        one = jax.random.randint(rng, (), max(1, total - bound), min(bound, total - 1) + 1)
        return jnp.stack([one, total - one])
    tallies = jnp.asarray(length_profile(amount, total, bound, skew), jnp.int32)
    couples = (amount - 1) // 2
    donor, sink = tallies[1:1 + 2 * couples:2], tallies[2:2 + 2 * couples:2]
    margin = jnp.minimum(donor - 1, bound - sink)
    passed = jax.random.randint(jax.random.fold_in(rng, 1), (couples,), 0, 1 << 20) % (margin + 1)
    tallies = tallies.at[1:1 + 2 * couples:2].set(donor - passed).at[2:2 + 2 * couples:2].set(sink + passed)
    return tallies[jax.random.permutation(jax.random.fold_in(rng, 2), amount)]


def bell_draw(key, shape, scale, most, cuts=(), kind=jnp.bfloat16):
    result = scale * jax.random.normal(key, shape, jnp.float32)
    if cuts:
        result = result * steps_of(key, shape, cuts, -0.22, 0.18)
    return jnp.clip(result, -most, most).astype(kind)


def setup_inputs(seed: int = 0) -> dict:
    streams_of = jax.random.split(jax.random.key(seed), 9)
    return {
        "amplitudes": bell_draw(streams_of[0], (NPAIR, NEXT, NEXT), 1.0, 6.0, ((0, 8), (1, 64))),
        "virtuals": bell_draw(streams_of[1], (NAO, NEXT), 300 ** -0.5, 0.375),
        "energies": jnp.clip(jnp.exp(jax.random.uniform(streams_of[2], (NEXT,), jnp.float32, math.log(0.02), math.log(0.2))), 0.02, 0.2),
        "integrals": bell_draw(streams_of[3], (NBLK * SHELL_ROW * SHELL_COL, KSCR * SHELL_ROW * SHELL_COL), (KSCR * SHELL_ROW * SHELL_COL) ** -0.5, 0.125, ((0, 64),)),
        "screened": draw_screened(jax.random.fold_in(streams_of[8], 71), 0),
        "counts": ragged_sizes(streams_of[5], NBLK, NBLK * KSCR // 2, KSCR, 2).astype(jnp.int32),
        "offsets": set_ends(jax.random.randint(streams_of[6], (2, NBLK), 0, NAO - SHELL_COL + 1), jax.random.fold_in(streams_of[6], 1), 0, NAO - SHELL_COL).astype(jnp.int32),
        "coupling": bell_draw(streams_of[7], (NPAIR, NPAIR), NPAIR ** -0.5, 0.5, ((0, 8),)),
    }


def reference(amplitudes, virtuals, energies, integrals, screened, counts, offsets, coupling):
    width = SHELL_ROW * SHELL_COL
    rows = offsets[0][:, None] + jnp.arange(SHELL_ROW, dtype=jnp.int32)[None, :]
    cols = offsets[1][:, None] + jnp.arange(SHELL_COL, dtype=jnp.int32)[None, :]
    left = virtuals[rows].astype(jnp.float32)
    right = virtuals[cols].astype(jnp.float32)

    def back(amp):
        half = jnp.dot(amp, virtuals.T, preferred_element_type=jnp.float32).astype(jnp.bfloat16)
        half = lax.optimization_barrier(half).astype(jnp.float32)
        picked = half[:, cols]
        blocks = jnp.einsum('bia,abs->bis', left, picked)
        return blocks.reshape(NBLK, width).astype(jnp.bfloat16)

    ao = lax.map(back, amplitudes)
    live = (jnp.arange(KSCR, dtype=jnp.int32)[None, :] < counts[:, None]).astype(jnp.float32)
    chosen = ao[:, screened, :].astype(jnp.float32) * live[None, :, :, None]
    slab = integrals.astype(jnp.float32).reshape(NBLK, width, KSCR, width)
    raw = jnp.einsum('jrkc,pjkc->pjr', slab, chosen).astype(jnp.bfloat16)
    mixed = jnp.einsum('pq,qjr->pjr', coupling.astype(jnp.float32), raw.astype(jnp.float32)).astype(jnp.bfloat16)
    diag = energies[:, None] + energies[None, :]

    def forward(pair):
        kmix, amp = pair
        square = kmix.astype(jnp.float32).reshape(NBLK, SHELL_ROW, SHELL_COL)
        upper = jnp.einsum('bia,bis->abs', left, square).astype(jnp.bfloat16)
        upper = lax.optimization_barrier(upper).astype(jnp.float32)
        inner = jnp.einsum('abs,bsn->an', upper, right)
        return (inner + diag * amp.astype(jnp.float32)).astype(jnp.bfloat16)

    return lax.map(forward, (mixed, amplitudes))
```

```python
import functools

import jax
import jax.numpy as jnp
from jax import lax
from jax.experimental import pallas as pl
from jax.experimental.pallas import tpu as pltpu
from jax.sharding import PartitionSpec as P

ROW = 8
COL = 16
WIDTH = ROW * COL
LANES = 128
GROUP = LANES // COL
BF = jnp.bfloat16
F32 = jnp.float32
MESH = pl.DeviceIdType.MESH
PAD = 24
VMEM_LIMIT = 60 * 1024 * 1024


def permutation(size):
    row = lax.broadcasted_iota(jnp.int32, (size, size), 0)
    col = lax.broadcasted_iota(jnp.int32, (size, size), 1)
    target = ((row // COL) % GROUP) * LANES + (row // LANES) * COL + row % COL
    return jnp.where(col == target, 1.0, 0.0).astype(BF)


def project_kernel(off, amp, virt, part, right, spread_e, vf, half, lrows, lt, spread_a, cells, stacked):
    nao, next_ = virt.shape
    rows = amp.shape[0]
    pairs = rows // COL
    nblk = off.shape[1]
    groups = nblk // GROUP
    me = lax.axis_index("sp")
    tile0 = me * COL // LANES
    sub0 = pl.multiple_of((me * COL) % LANES, COL)

    chunk = 128
    whole = nao // chunk

    def widen(c, _):
        at = pl.multiple_of(c * chunk, chunk)
        for t in range(next_ // LANES):
            vf[t, pl.ds(at, chunk), :] = virt[pl.ds(at, chunk), t * LANES : (t + 1) * LANES].astype(F32)
        return 0

    lax.fori_loop(0, whole, widen, 0)
    if nao % chunk:
        for t in range(next_ // LANES):
            vf[t, whole * chunk : nao, :] = virt[whole * chunk : nao, t * LANES : (t + 1) * LANES].astype(F32)

    def pick(b, _):
        to = pl.multiple_of(b * COL, COL)
        for t in range(next_ // LANES):
            right[pl.ds(to, COL), t * LANES : (t + 1) * LANES] = vf[t, pl.ds(off[1, b], COL), :].astype(BF)
        lrows[pl.ds(pl.multiple_of(b * ROW, ROW), ROW), :] = vf[tile0, pl.ds(off[0, b], ROW), :]
        return 0

    lax.fori_loop(0, nblk, pick, 0)

    owner = lax.broadcasted_iota(jnp.int32, (nblk, nblk * COL), 1) // COL
    repeat = jnp.where(lax.broadcasted_iota(jnp.int32, (nblk, nblk * COL), 0) == owner, 1.0, 0.0).astype(BF)
    for i in range(ROW):
        lt[...] = lrows[pl.ds(i, nblk, stride=ROW), :].T
        mine = jnp.dot(lt[pl.ds(sub0, COL), :].astype(BF), repeat, preferred_element_type=F32)
        spread_e[i * COL : (i + 1) * COL, :] = mine
        for g in range(groups):
            spread_a[g, pl.ds(i, COL, stride=ROW), :] = mine[:, g * LANES : (g + 1) * LANES]

    step = 256
    for n in range(0, nblk * COL, step):
        got = lax.dot_general(
            amp[...], right[n : n + step, :], (((1,), (1,)), ((), ())), preferred_element_type=F32
        )
        got = got.astype(BF).astype(F32)
        for t in range(step // LANES):
            half[n // LANES + t] = got[:, t * LANES : (t + 1) * LANES]

    cells[...] = jnp.zeros_like(cells)
    for g in range(groups):

        def contract(p, _):
            total = jnp.zeros((ROW, LANES), F32)
            for a in range(COL):
                line = half[g, pl.ds(p * COL + a, ROW, stride=0), :]
                total = total + spread_a[g, a * ROW : (a + 1) * ROW, :] * line
            cells[pl.ds(pl.multiple_of(g * PAD * ROW + p * ROW, ROW), ROW), :] = total
            return 0

        lax.fori_loop(0, pairs, contract, 0, unroll=2)
        for i in range(ROW):
            stacked[g * PAD : (g + 1) * PAD, i * LANES : (i + 1) * LANES] = cells[
                pl.ds(g * PAD * ROW + i, PAD, stride=ROW), :
            ]
    moved = jnp.dot(stacked[...].astype(BF), permutation(GROUP * LANES), preferred_element_type=F32)
    for g in range(groups):
        for v in range(GROUP):
            part[v % 2, (g * GROUP + v) // 2] = moved[
                g * PAD : g * PAD + pairs, v * LANES : (v + 1) * LANES
            ].astype(BF)


def project(offsets, amp, virtuals, pairs):
    nao, next_ = virtuals.shape
    nblk = offsets.shape[1]
    rows = amp.shape[0]
    groups = nblk // GROUP
    vmem = pl.BlockSpec(memory_space=pltpu.VMEM)
    return pl.pallas_call(
        project_kernel,
        out_shape=(
            jax.ShapeDtypeStruct((2, nblk // 2, pairs, WIDTH), BF),
            jax.ShapeDtypeStruct((nblk * COL, next_), BF),
            jax.ShapeDtypeStruct((ROW * COL, nblk * COL), F32),
        ),
        in_specs=[pl.BlockSpec(memory_space=pltpu.SMEM), vmem, vmem],
        out_specs=(vmem, vmem, vmem),
        scratch_shapes=[
            pltpu.VMEM((next_ // LANES, nao, LANES), F32),
            pltpu.VMEM((groups, rows, LANES), F32),
            pltpu.VMEM((nblk * ROW, LANES), F32),
            pltpu.VMEM((LANES, nblk), F32),
            pltpu.VMEM((groups, COL * ROW, LANES), F32),
            pltpu.VMEM((groups * PAD * ROW, LANES), F32),
            pltpu.VMEM((groups * PAD, ROW * LANES), F32),
        ],
        compiler_params=pltpu.CompilerParams(vmem_limit_bytes=VMEM_LIMIT),
        name="project",
    )(offsets, amp, virtuals)


def far_first(t, size):
    return size // 2 + (1 - 2 * (t % 2)) * ((t + 1) // 2)


def exchange_kernel(
    nx, ny,
    screened, counts, part, integrals, coupling, mixed_all,
    pairsum, outgoing, arrived, ao_own, ao_all, chosen, raw_own, raw_all, raw_rows, mix_own,
    pair_s, pair_r, rs_s, rs_r, ag_s, ag_r, fw_s, fw_r, z_s, z_r, mg_s, mg_r, mf_s, mf_r,
):
    sp = lax.axis_index("sp")
    z = lax.axis_index("pb")
    nz = lax.axis_size("pb")
    core = sp % 2
    chip = sp // 2
    x = chip % nx
    y = chip // nx
    chips = nx * ny
    other = (chip * 2 + (1 - core), z)
    pairs = ao_own.shape[0]

    def peer(t):
        dy = far_first(t // nx, ny)
        dx = far_first(t % nx, nx)
        return ((y + dy) % ny) * nx + (x + dx) % nx

    def source(t):
        dy = far_first(t // nx, ny)
        dx = far_first(t % nx, nx)
        return ((y + ny - dy) % ny) * nx + (x + nx - dx) % nx

    barrier = pltpu.get_barrier_semaphore()
    pl.semaphore_signal(barrier, inc=1, device_id=other, device_id_type=MESH)

    def greet(t, _):
        pl.semaphore_signal(barrier, inc=1, device_id=(peer(t) * 2 + core, z), device_id_type=MESH)
        return 0

    lax.fori_loop(0, chips - 1, greet, 0)

    def greet_z(t, _):
        pl.semaphore_signal(barrier, inc=1, device_id=(sp, (z + 1 + t) % nz), device_id_type=MESH)
        return 0

    lax.fori_loop(0, nz - 1, greet_z, 0)
    pl.semaphore_wait(barrier, chips + nz - 1)

    swap = pltpu.make_async_remote_copy(
        part.at[1 - core], pairsum, pair_s, pair_r, device_id=other, device_id_type=MESH
    )
    swap.start()
    swap.wait_recv()
    outgoing[...] = (part[core].astype(F32) + pairsum[...].astype(F32)).astype(BF)

    def scatter(t):
        to = peer(t)
        return pltpu.make_async_remote_copy(
            outgoing.at[to], arrived.at[chip], rs_s.at[t], rs_r.at[t],
            device_id=(to * 2 + core, z), device_id_type=MESH,
        )

    def scatter_wait(t, total):
        come = source(t)
        pltpu.make_async_remote_copy(
            outgoing.at[come], arrived.at[come], rs_s.at[t], rs_r.at[t],
            device_id=(come * 2 + core, z), device_id_type=MESH,
        ).wait_recv()
        return total + arrived[come].astype(F32)

    def go(t, _):
        scatter(t).start()
        return 0

    lax.fori_loop(0, chips - 1, go, 0)
    total = lax.fori_loop(0, chips - 1, lambda t, c: scatter_wait(chips - 2 - t, c), outgoing[chip].astype(F32))
    ao_own[...] = total.astype(BF)

    def gather(own, landing, send, recv, fsend, frecv):
        def to_peer(t):
            return pltpu.make_async_remote_copy(
                own, landing.at[core, chip], send.at[t], recv.at[t],
                device_id=(peer(t) * 2 + core, z), device_id_type=MESH,
            )

        def from_peer(t):
            come = source(t)
            return pltpu.make_async_remote_copy(
                own, landing.at[core, come], send.at[t], recv.at[t],
                device_id=(come * 2 + core, z), device_id_type=MESH,
            )

        def forward(t):
            come = source(t)
            return pltpu.make_async_remote_copy(
                landing.at[core, come], landing.at[core, come], fsend.at[t], frecv.at[t],
                device_id=other, device_id_type=MESH,
            )

        def from_other(t):
            come = source(t)
            return pltpu.make_async_remote_copy(
                landing.at[1 - core, come], landing.at[1 - core, come], fsend.at[t], frecv.at[t],
                device_id=other, device_id_type=MESH,
            )

        def begin(t, _):
            to_peer(t).start()
            return 0

        lax.fori_loop(0, chips - 1, begin, 0)
        mine = pltpu.make_async_remote_copy(
            own, landing.at[core, chip], fsend.at[chips - 1], frecv.at[chips - 1],
            device_id=other, device_id_type=MESH,
        )
        mine.start()
        landing[core, chip] = own[...]

        def relay(t, _):
            u = chips - 2 - t
            from_peer(u).wait_recv()
            forward(u).start()
            return 0

        lax.fori_loop(0, chips - 1, relay, 0)
        pltpu.make_async_remote_copy(
            own, landing.at[1 - core, chip], fsend.at[chips - 1], frecv.at[chips - 1],
            device_id=other, device_id_type=MESH,
        ).wait_recv()

        def settle(t, _):
            from_other(chips - 2 - t).wait_recv()
            return 0

        lax.fori_loop(0, chips - 1, settle, 0)

        def drain():
            def one(t, _):
                to_peer(t).wait_send()
                forward(t).wait_send()
                return 0

            lax.fori_loop(0, chips - 1, one, 0)
            mine.wait_send()

        return drain

    drain_ao = gather(ao_own, ao_all, ag_s, ag_r, fw_s, fw_r)

    slots = screened.shape[1]
    for k in range(slots):
        b = screened[0, k]
        tile = ao_all[b % 2, b // 2].astype(F32)
        chosen[:, k * WIDTH : (k + 1) * WIDTH] = jnp.where(k < counts[0], tile, 0.0).astype(BF)
    raw = lax.dot_general(
        chosen[...], integrals[...], (((1,), (1,)), ((), ())), preferred_element_type=F32
    )
    raw_own[...] = raw.astype(BF)

    def along(t):
        return pltpu.make_async_remote_copy(
            raw_own, raw_all.at[z], z_s.at[t], z_r.at[t],
            device_id=(sp, (z + far_first(t, nz)) % nz), device_id_type=MESH,
        )

    def along_in(t):
        come = (z + nz - far_first(t, nz)) % nz
        return pltpu.make_async_remote_copy(
            raw_own, raw_all.at[come], z_s.at[t], z_r.at[t],
            device_id=(sp, come), device_id_type=MESH,
        )

    for t in range(nz - 1):
        along(t).start()
    raw_all[z] = raw_own[...]
    for t in range(nz - 1):
        along_in(t).wait_recv()
    for q in range(nz):
        raw_rows[q * pairs : (q + 1) * pairs, :] = raw_all[q].astype(F32)
    mix = jnp.dot(coupling[...], raw_rows[...].astype(BF), preferred_element_type=F32)
    mix_own[...] = mix.astype(BF)

    drain_mix = gather(mix_own, mixed_all, mg_s, mg_r, mf_s, mf_r)

    swap.wait_send()

    def drain_rs(t, _):
        scatter(t).wait_send()
        return 0

    lax.fori_loop(0, chips - 1, drain_rs, 0)
    drain_ao()
    for t in range(nz - 1):
        along(t).wait_send()
    drain_mix()


def exchange(screened, counts, part, integrals, coupling, nx, ny, nz):
    _, chips, pairs, width = part.shape
    slots = screened.shape[1]
    vmem = pl.BlockSpec(memory_space=pltpu.VMEM)
    smem = pl.BlockSpec(memory_space=pltpu.SMEM)
    dma = pltpu.SemaphoreType.DMA
    return pl.pallas_call(
        functools.partial(exchange_kernel, nx, ny),
        out_shape=jax.ShapeDtypeStruct(part.shape, BF),
        in_specs=[smem, smem, vmem, vmem, vmem],
        out_specs=vmem,
        scratch_shapes=[
            pltpu.VMEM((chips, pairs, width), BF),
            pltpu.VMEM((chips, pairs, width), BF),
            pltpu.VMEM((chips, pairs, width), BF),
            pltpu.VMEM((pairs, width), BF),
            pltpu.VMEM((2, chips, pairs, width), BF),
            pltpu.VMEM((pairs, slots * width), BF),
            pltpu.VMEM((pairs, width), BF),
            pltpu.VMEM((nz, pairs, width), BF),
            pltpu.VMEM((nz * pairs, width), F32),
            pltpu.VMEM((pairs, width), BF),
            dma, dma,
            dma((chips,)), dma((chips,)),
            dma((chips,)), dma((chips,)), dma((chips,)), dma((chips,)),
            dma((nz,)), dma((nz,)),
            dma((chips,)), dma((chips,)), dma((chips,)), dma((chips,)),
        ],
        compiler_params=pltpu.CompilerParams(
            collective_id=0, has_side_effects=True, vmem_limit_bytes=VMEM_LIMIT
        ),
        name="exchange",
    )(screened, counts, part, integrals, coupling)


def finish_kernel(mixed_all, right, spread_e, amp, energies, out, blocks, cells, upper):
    _, chips, pairs, _ = mixed_all.shape
    rows, next_ = amp.shape
    groups = chips * 2 // GROUP
    me = lax.axis_index("sp")
    blocks[...] = jnp.zeros_like(blocks)
    for g in range(groups):
        for v in range(GROUP):
            blocks[g * PAD : g * PAD + pairs, v * LANES : (v + 1) * LANES] = mixed_all[
                v % 2, (g * GROUP + v) // 2
            ].astype(F32)
    moved = jnp.dot(blocks[...].astype(BF), permutation(GROUP * LANES), preferred_element_type=F32)
    for i in range(ROW):
        cells[i] = moved[:, i * LANES : (i + 1) * LANES]
    for g in range(groups):
        lanes = slice(g * LANES, (g + 1) * LANES)

        def lift(p, _):
            total = jnp.zeros((COL, LANES), F32)
            for i in range(ROW):
                line = cells[i, pl.ds(g * PAD + p, ROW, stride=0), :]
                line = jnp.concatenate([line, line], axis=0)
                total = total + spread_e[i * COL : (i + 1) * COL, lanes] * line
            upper[pl.ds(pl.multiple_of(p * COL, COL), COL), lanes] = total.astype(BF)
            return 0

        lax.fori_loop(0, pairs, lift, 0, unroll=2)
    hit = lax.broadcasted_iota(jnp.int32, (COL, next_), 1) == (
        lax.broadcasted_iota(jnp.int32, (COL, next_), 0) + me * COL
    )
    own = jnp.sum(jnp.where(hit, energies[...], 0.0), axis=1, keepdims=True)
    step = 256
    for n in range(0, next_, step):
        inner = jnp.dot(upper[...], right[:, n : n + step], preferred_element_type=F32)
        diag = own + energies[:, n : n + step]
        term = amp[:, n : n + step].astype(F32).reshape(pairs, COL, step) * diag[None]
        out[:, n : n + step] = (inner + term.reshape(rows, step)).astype(BF)


def finish(mixed_all, right, spread_e, amp, energies):
    _, chips, pairs, _ = mixed_all.shape
    groups = chips * 2 // GROUP
    vmem = pl.BlockSpec(memory_space=pltpu.VMEM)
    return pl.pallas_call(
        finish_kernel,
        out_shape=jax.ShapeDtypeStruct(amp.shape, BF),
        in_specs=[vmem] * 5,
        out_specs=vmem,
        scratch_shapes=[
            pltpu.VMEM((groups * PAD, GROUP * LANES), F32),
            pltpu.VMEM((ROW, groups * PAD, LANES), F32),
            pltpu.VMEM((amp.shape[0], groups * LANES), BF),
        ],
        compiler_params=pltpu.CompilerParams(vmem_limit_bytes=VMEM_LIMIT),
        name="finish",
    )(mixed_all, right, spread_e, amp, energies)


NX, NY, NZ = 4, 8, 8


def shards(amplitudes, virtuals, energies, integrals, screened, counts, offsets, coupling):
    pairs, ext, next_ = amplitudes.shape
    amp = amplitudes.reshape(pairs * ext, next_)
    part, right, spread_e = project(offsets, amp, virtuals, pairs)
    mixed_all = exchange(screened, counts, part, integrals, coupling, NX, NY, NZ)
    out = finish(mixed_all, right, spread_e, amp, energies.reshape(1, next_))
    return out.reshape(pairs, ext, next_)


def solution(mesh):
    return jax.shard_map(
        shards,
        mesh=mesh,
        in_specs=(
            P("pb", "sp", None),
            P(),
            P(),
            P("sp", None),
            P("sp", None),
            P("sp"),
            P(),
            P("pb", None),
        ),
        out_specs=P("pb", "sp", None),
        check_vma=False,
    )
```

```python
import functools

import jax
import jax.numpy as jnp
from jax import lax
from jax.experimental import pallas as pl
from jax.experimental.pallas import tpu as pltpu
from jax.sharding import PartitionSpec as P

ROW = 8
COL = 16
WIDTH = ROW * COL
LANES = 128
GROUP = LANES // COL
SUB = 4
BF = jnp.bfloat16
F32 = jnp.float32
MESH = pl.DeviceIdType.MESH
PAD = 24
VROWS = 176
NX, NY = 4, 8


def far_first(t, size):
    return size // 2 + (1 - 2 * (t % 2)) * ((t + 1) // 2)


def residual_kernel(
    off, screened, counts, virt, amp_hbm, integrals_hbm, coupling, energies, out,
    right, upper, diag, vbuf, vf, amp, integrals, perm, half, lrows, lt, spread_e, spread_a, cells, stacked,
    part, pairsum, outgoing, arrived, ao_own, ao_all, chosen, raw_own, raw_all, raw_rows, mix_own, mixed_all,
    local_s, pair_s, pair_r, rs_s, rs_r, ag_s, ag_r, fw_s, fw_r, z_s, z_r, mg_s, mg_r, mf_s, mf_r,
):
    nao, next_ = virt.shape
    rows = amp.shape[0]
    pairs = rows // COL
    pieces = pairs // SUB
    nblk = off.shape[1]
    groups = nblk // GROUP
    tiles = next_ // LANES
    slots = screened.shape[1]
    chips = NX * NY

    sp = lax.axis_index("sp")
    z = lax.axis_index("pb")
    nz = lax.axis_size("pb")
    core = sp % 2
    chip = sp // 2
    x = chip % NX
    y = chip // NX
    other = (chip * 2 + (1 - core), z)

    def peer(t):
        dy = far_first(t // NX, NY)
        dx = far_first(t % NX, NX)
        return ((y + dy) % NY) * NX + (x + dx) % NX

    def source(t):
        dy = far_first(t // NX, NY)
        dx = far_first(t % NX, NX)
        return ((y + NY - dy) % NY) * NX + (x + NX - dx) % NX

    barrier = pltpu.get_barrier_semaphore()

    def greet(t, _):
        pl.semaphore_signal(barrier, inc=1, device_id=(peer(t) * 2 + core, z), device_id_type=MESH)
        return 0

    lax.fori_loop(0, chips - 1, greet, 0)

    def greet_z(t, _):
        pl.semaphore_signal(barrier, inc=1, device_id=(sp, (z + 1 + t) % nz), device_id_type=MESH)
        return 0

    lax.fori_loop(0, nz - 1, greet_z, 0)
    pl.semaphore_signal(barrier, inc=1, device_id=other, device_id_type=MESH)

    starts = list(range(0, nao, VROWS))
    loads = []
    for c, at in enumerate(starts):
        size = min(VROWS, nao - at)
        loads.append(
            pltpu.make_async_copy(virt.at[pl.ds(at, size)], vbuf.at[pl.ds(at, size)], local_s.at[c])
        )
    amp_load = pltpu.make_async_copy(amp_hbm, amp, local_s.at[len(starts)])
    int_load = pltpu.make_async_copy(integrals_hbm, integrals, local_s.at[len(starts) + 1])
    for load in loads:
        load.start()
    amp_load.start()
    int_load.start()

    def mark(u, _):
        shape = (LANES, GROUP * LANES)
        row = lax.broadcasted_iota(jnp.int32, shape, 0)
        col = lax.broadcasted_iota(jnp.int32, shape, 1)
        target = (row // COL) * LANES + u * COL + row % COL
        perm[pl.ds(pl.multiple_of(u * LANES, LANES), LANES), :] = jnp.where(col == target, 1.0, 0.0).astype(BF)
        return 0

    lax.fori_loop(0, GROUP, mark, 0)
    cells[...] = jnp.zeros_like(cells)

    for c, at in enumerate(starts):
        size = min(VROWS, nao - at)
        loads[c].wait()
        for t in range(tiles):
            vf[t, at : at + size, :] = vbuf[at : at + size, t * LANES : (t + 1) * LANES].astype(F32)

    tile0 = sp * COL // LANES
    sub0 = pl.multiple_of((sp * COL) % LANES, COL)

    def pick(b, _):
        to = pl.multiple_of(b * COL, COL)
        for t in range(tiles):
            right[pl.ds(to, COL), t * LANES : (t + 1) * LANES] = vf[t, pl.ds(off[1, b], COL), :].astype(BF)
        lrows[pl.ds(pl.multiple_of(b * ROW, ROW), ROW), :] = vf[tile0, pl.ds(off[0, b], ROW), :]
        return 0

    lax.fori_loop(0, nblk, pick, 0, unroll=2)

    owner = lax.broadcasted_iota(jnp.int32, (nblk, nblk * COL), 1) // COL
    repeat = jnp.where(lax.broadcasted_iota(jnp.int32, (nblk, nblk * COL), 0) == owner, 1.0, 0.0).astype(BF)
    for i in range(ROW):
        lt[i] = lrows[pl.ds(i, nblk, stride=ROW), :].T
        mine = jnp.dot(lt[i, pl.ds(sub0, COL), :].astype(BF), repeat, preferred_element_type=F32)
        spread_e[i * COL : (i + 1) * COL, :] = mine
        for g in range(groups):
            spread_a[g, pl.ds(i, COL, stride=ROW), :] = mine[:, g * LANES : (g + 1) * LANES]

    amp_load.wait()
    step = 256
    for n in range(0, nblk * COL, step):
        got = lax.dot_general(
            amp[...], right[n : n + step, :], (((1,), (1,)), ((), ())), preferred_element_type=F32
        )
        got = got.astype(BF).astype(F32)
        for t in range(step // LANES):
            half[n // LANES + t] = got[:, t * LANES : (t + 1) * LANES]

    for g in range(groups):

        def contract(p, _):
            total = jnp.zeros((ROW, LANES), F32)
            for a in range(COL):
                line = half[g, pl.ds(p * COL + a, ROW, stride=0), :]
                total = total + spread_a[g, a * ROW : (a + 1) * ROW, :] * line
            cells[pl.ds(pl.multiple_of(g * PAD * ROW + p * ROW, ROW), ROW), :] = total
            return 0

        lax.fori_loop(0, pairs, contract, 0, unroll=2)
        for i in range(ROW):
            stacked[g * PAD : (g + 1) * PAD, i * LANES : (i + 1) * LANES] = cells[
                pl.ds(g * PAD * ROW + i, PAD, stride=ROW), :
            ].astype(BF)
    moved = jnp.dot(stacked[...], perm[...], preferred_element_type=F32)
    for g in range(groups):
        for v in range(GROUP):
            for j in range(pieces):
                part[v % 2, (g * GROUP + v) // 2, j] = moved[
                    g * PAD + j * SUB : g * PAD + (j + 1) * SUB, v * LANES : (v + 1) * LANES
                ].astype(BF)

    hit = lax.broadcasted_iota(jnp.int32, (COL, next_), 1) == (
        lax.broadcasted_iota(jnp.int32, (COL, next_), 0) + sp * COL
    )
    own_energy = jnp.sum(jnp.where(hit, energies[...], 0.0), axis=1, keepdims=True)

    pl.semaphore_wait(barrier, chips + nz - 1)

    def swap(t):
        to = peer(t)
        return pltpu.make_async_remote_copy(
            part.at[1 - core, to], pairsum.at[to], pair_s.at[t], pair_r.at[t],
            device_id=other, device_id_type=MESH,
        )

    def scatter(t):
        to = peer(t)
        return pltpu.make_async_remote_copy(
            outgoing.at[to], arrived.at[chip], rs_s.at[t], rs_r.at[t],
            device_id=(to * 2 + core, z), device_id_type=MESH,
        )

    def swap_go(t, _):
        swap(t).start()
        return 0

    def pair_total(t):
        to = peer(t)
        swap(t).wait_recv()
        return part[core, to].astype(F32) + pairsum[to].astype(F32)

    def scatter_go(t, _):
        outgoing[peer(t)] = pair_total(t).astype(BF)
        scatter(t).start()
        return 0

    def scatter_in(t, total):
        u = chips - 2 - t
        come = source(u)
        pltpu.make_async_remote_copy(
            outgoing.at[come], arrived.at[come], rs_s.at[u], rs_r.at[u],
            device_id=(come * 2 + core, z), device_id_type=MESH,
        ).wait_recv()
        return total + arrived[come].astype(F32)

    lax.fori_loop(0, chips, swap_go, 0)
    lax.fori_loop(0, chips - 1, scatter_go, 0)

    def diagonal(p, _):
        at = pl.multiple_of(p * COL, COL)
        diag[pl.ds(at, COL), :] = (own_energy + energies[...]) * amp[pl.ds(at, COL), :].astype(F32)
        return 0

    lax.fori_loop(0, pairs, diagonal, 0)
    total = lax.fori_loop(0, chips - 1, scatter_in, pair_total(chips - 1))
    ao_own[...] = total.astype(BF)

    def gather(own, landing, send, recv, fsend, frecv):
        def to_peer(t):
            return pltpu.make_async_remote_copy(
                own, landing.at[core, chip], send.at[t], recv.at[t],
                device_id=(peer(t) * 2 + core, z), device_id_type=MESH,
            )

        def from_peer(t):
            come = source(t)
            return pltpu.make_async_remote_copy(
                own, landing.at[core, come], send.at[t], recv.at[t],
                device_id=(come * 2 + core, z), device_id_type=MESH,
            )

        def forward(t):
            come = source(t)
            return pltpu.make_async_remote_copy(
                landing.at[core, come], landing.at[core, come], fsend.at[t], frecv.at[t],
                device_id=other, device_id_type=MESH,
            )

        def from_other(t):
            come = source(t)
            return pltpu.make_async_remote_copy(
                landing.at[1 - core, come], landing.at[1 - core, come], fsend.at[t], frecv.at[t],
                device_id=other, device_id_type=MESH,
            )

        def begin(t, _):
            to_peer(t).start()
            return 0

        lax.fori_loop(0, chips - 1, begin, 0)
        mine = pltpu.make_async_remote_copy(
            own, landing.at[core, chip], fsend.at[chips - 1], frecv.at[chips - 1],
            device_id=other, device_id_type=MESH,
        )
        mine.start()
        landing[core, chip] = own[...]

        def relay(t, _):
            u = chips - 2 - t
            from_peer(u).wait_recv()
            forward(u).start()
            return 0

        lax.fori_loop(0, chips - 1, relay, 0)
        pltpu.make_async_remote_copy(
            own, landing.at[1 - core, chip], fsend.at[chips - 1], frecv.at[chips - 1],
            device_id=other, device_id_type=MESH,
        ).wait_recv()

        def settle(t, _):
            from_other(chips - 2 - t).wait_recv()
            return 0

        lax.fori_loop(0, chips - 1, settle, 0)

        def drain():
            def one(t, _):
                to_peer(t).wait_send()
                forward(t).wait_send()
                return 0

            lax.fori_loop(0, chips - 1, one, 0)
            mine.wait_send()

        return drain

    drain_ao = gather(ao_own, ao_all, ag_s, ag_r, fw_s, fw_r)

    for k in range(slots):
        b = screened[0, k]
        tile = jnp.where(k < counts[0], ao_all[b % 2, b // 2].astype(F32), 0.0)
        for j in range(pieces):
            chosen[j * SUB : (j + 1) * SUB, k * WIDTH : (k + 1) * WIDTH] = tile[j]
    int_load.wait()
    raw = lax.dot_general(
        chosen[...].astype(BF), integrals[...], (((1,), (1,)), ((), ())), preferred_element_type=F32
    )
    for j in range(pieces):
        raw_own[j] = raw[j * SUB : (j + 1) * SUB, :].astype(BF)

    def along(t):
        return pltpu.make_async_remote_copy(
            raw_own, raw_all.at[z], z_s.at[t], z_r.at[t],
            device_id=(sp, (z + far_first(t, nz)) % nz), device_id_type=MESH,
        )

    def along_in(t):
        come = (z + nz - far_first(t, nz)) % nz
        return pltpu.make_async_remote_copy(
            raw_own, raw_all.at[come], z_s.at[t], z_r.at[t],
            device_id=(sp, come), device_id_type=MESH,
        )

    for t in range(nz - 1):
        along(t).start()
    raw_all[z] = raw_own[...]
    for t in range(nz - 1):
        along_in(t).wait_recv()
    for q in range(nz):
        for j in range(pieces):
            at = q * pairs + j * SUB
            raw_rows[at : at + SUB, :] = raw_all[q, j].astype(F32)
    mix = jnp.dot(coupling[...], raw_rows[...].astype(BF), preferred_element_type=F32)
    for j in range(pieces):
        mix_own[j] = mix[j * SUB : (j + 1) * SUB, :].astype(BF)

    drain_mix = gather(mix_own, mixed_all, mg_s, mg_r, mf_s, mf_r)

    for b in range(nblk):
        block = mixed_all[b % 2, b // 2].astype(F32)
        for j in range(pieces):
            cells[b * PAD + j * SUB : b * PAD + (j + 1) * SUB, :] = block[j]
    for g in range(groups):
        for v in range(GROUP):
            at = (g * GROUP + v) * PAD
            stacked[g * PAD : (g + 1) * PAD, v * LANES : (v + 1) * LANES] = cells[at : at + PAD, :].astype(BF)
    moved = jnp.dot(stacked[...], perm[...], preferred_element_type=F32)
    for i in range(ROW):
        cells[i * groups * PAD : (i + 1) * groups * PAD, :] = moved[:, i * LANES : (i + 1) * LANES]
    for g in range(groups):
        lanes = slice(g * LANES, (g + 1) * LANES)

        def lift(p, _):
            total = jnp.zeros((COL, LANES), F32)
            for i in range(ROW):
                line = cells[pl.ds(i * groups * PAD + g * PAD + p, ROW, stride=0), :]
                line = jnp.concatenate([line, line], axis=0)
                total = total + spread_e[i * COL : (i + 1) * COL, lanes] * line
            upper[pl.ds(pl.multiple_of(p * COL, COL), COL), lanes] = total.astype(BF)
            return 0

        lax.fori_loop(0, pairs, lift, 0, unroll=2)

    step = 256
    for n in range(0, next_, step):
        inner = jnp.dot(upper[...], right[:, n : n + step], preferred_element_type=F32)
        out[:, n : n + step] = (inner + diag[:, n : n + step]).astype(BF)

    def drain_rs(t, _):
        swap(t).wait_send()
        scatter(t).wait_send()
        return 0

    lax.fori_loop(0, chips - 1, drain_rs, 0)
    swap(chips - 1).wait_send()
    drain_ao()
    for t in range(nz - 1):
        along(t).wait_send()
    drain_mix()


def residual(offsets, screened, counts, virtuals, amp, integrals, coupling, energies, nz):
    nao, next_ = virtuals.shape
    rows = amp.shape[0]
    pairs = rows // COL
    pieces = pairs // SUB
    nblk = offsets.shape[1]
    groups = nblk // GROUP
    chips = NX * NY
    slots = screened.shape[1]
    vmem = pl.BlockSpec(memory_space=pltpu.VMEM)
    smem = pl.BlockSpec(memory_space=pltpu.SMEM)
    hbm = pl.BlockSpec(memory_space=pltpu.HBM)
    dma = pltpu.SemaphoreType.DMA
    message = (pieces, SUB, WIDTH)
    return pl.pallas_call(
        residual_kernel,
        out_shape=jax.ShapeDtypeStruct((rows, next_), BF),
        in_specs=[smem, smem, smem, hbm, hbm, hbm, vmem, vmem],
        out_specs=vmem,
        scratch_shapes=[
            pltpu.VMEM((nblk * COL, next_), BF),
            pltpu.VMEM((rows, nblk * COL), BF),
            pltpu.VMEM((rows, next_), F32),
            pltpu.VMEM((nao, next_), BF),
            pltpu.VMEM((next_ // LANES, nao, LANES), F32),
            pltpu.VMEM((rows, next_), BF),
            pltpu.VMEM(integrals.shape, BF),
            pltpu.VMEM((GROUP * LANES, GROUP * LANES), BF),
            pltpu.VMEM((groups, rows, LANES), F32),
            pltpu.VMEM((nblk * ROW, LANES), F32),
            pltpu.VMEM((ROW, LANES, nblk), F32),
            pltpu.VMEM((ROW * COL, nblk * COL), F32),
            pltpu.VMEM((groups, COL * ROW, LANES), F32),
            pltpu.VMEM((groups * PAD * ROW, LANES), F32),
            pltpu.VMEM((groups * PAD, ROW * LANES), BF),
            pltpu.VMEM((2, chips, *message), BF),
            pltpu.VMEM((chips, *message), BF),
            pltpu.VMEM((chips, *message), BF),
            pltpu.VMEM((chips, *message), BF),
            pltpu.VMEM(message, BF),
            pltpu.VMEM((2, chips, *message), BF),
            pltpu.VMEM((pairs, slots * WIDTH), F32),
            pltpu.VMEM(message, BF),
            pltpu.VMEM((nz, *message), BF),
            pltpu.VMEM((nz * pairs, WIDTH), F32),
            pltpu.VMEM(message, BF),
            pltpu.VMEM((2, chips, *message), BF),
            dma((-(-nao // VROWS) + 2,)),
            dma((chips,)), dma((chips,)),
            dma((chips,)), dma((chips,)),
            dma((chips,)), dma((chips,)), dma((chips,)), dma((chips,)),
            dma((nz,)), dma((nz,)),
            dma((chips,)), dma((chips,)), dma((chips,)), dma((chips,)),
        ],
        compiler_params=pltpu.CompilerParams(
            collective_id=0, has_side_effects=True, vmem_limit_bytes=58 * 1024 * 1024
        ),
        name="residual",
    )(offsets, screened, counts, virtuals, amp, integrals, coupling, energies)


def shards(amplitudes, virtuals, energies, integrals, screened, counts, offsets, coupling):
    pairs, ext, next_ = amplitudes.shape
    amp = amplitudes.reshape(pairs * ext, next_)
    nz = coupling.shape[1] // pairs
    out = residual(offsets, screened, counts, virtuals, amp, integrals, coupling, energies.reshape(1, next_), nz)
    return out.reshape(pairs, ext, next_)


def solution(mesh):
    return jax.shard_map(
        shards,
        mesh=mesh,
        in_specs=(
            P("pb", "sp", None),
            P(),
            P(),
            P("sp", None),
            P("sp", None),
            P("sp"),
            P(),
            P("pb", None),
        ),
        out_specs=P("pb", "sp", None),
        check_vma=False,
    )
```

```python
import functools

import jax
import jax.numpy as jnp
from jax import lax
from jax.experimental import pallas as pl
from jax.experimental.pallas import tpu as pltpu
from jax.sharding import PartitionSpec as P

ROW = 8
COL = 16
WIDTH = ROW * COL
LANES = 128
GROUP = LANES // COL
SUB = 4
BF = jnp.bfloat16
F32 = jnp.float32
MESH = pl.DeviceIdType.MESH
PAD = 24
VROWS = 176
NX, NY = 4, 8


def far_first(t, size):
    return size // 2 + (1 - 2 * (t % 2)) * ((t + 1) // 2)


def residual_kernel(
    off, screened, counts, virt, amp_hbm, integrals_hbm, coupling, energies, out,
    right, upper, diag, vbuf, vf, amp, integrals, perm, half, lrows, lt, spread_e, spread_a, cells, stacked,
    part, pairsum, outgoing, arrived, ao_own, ao_all, chosen, raw_own, raw_all, raw_rows, mix_own, mixed_all,
    local_s, pair_s, pair_r, rs_s, rs_r, ag_s, ag_r, fw_s, fw_r, z_s, z_r, mg_s, mg_r, mf_s, mf_r,
):
    nao, next_ = virt.shape
    rows = amp.shape[0]
    pairs = rows // COL
    pieces = pairs // SUB
    nblk = off.shape[1]
    groups = nblk // GROUP
    tiles = next_ // LANES
    slots = screened.shape[1]
    chips = NX * NY

    sp = lax.axis_index("sp")
    z = lax.axis_index("pb")
    nz = lax.axis_size("pb")
    core = sp % 2
    chip = sp // 2
    x = chip % NX
    y = chip // NX
    other = (chip * 2 + (1 - core), z)

    def peer(t):
        dy = far_first(t // NX, NY)
        dx = far_first(t % NX, NX)
        return ((y + dy) % NY) * NX + (x + dx) % NX

    barrier = pltpu.get_barrier_semaphore()

    def greet(t, _):
        pl.semaphore_signal(barrier, inc=1, device_id=(peer(t) * 2 + core, z), device_id_type=MESH)
        return 0

    lax.fori_loop(0, chips - 1, greet, 0)

    def greet_z(t, _):
        pl.semaphore_signal(barrier, inc=1, device_id=(sp, (z + 1 + t) % nz), device_id_type=MESH)
        return 0

    lax.fori_loop(0, nz - 1, greet_z, 0)
    pl.semaphore_signal(barrier, inc=1, device_id=other, device_id_type=MESH)

    starts = list(range(0, nao, VROWS))
    loads = []
    for c, at in enumerate(starts):
        size = min(VROWS, nao - at)
        loads.append(
            pltpu.make_async_copy(virt.at[pl.ds(at, size)], vbuf.at[pl.ds(at, size)], local_s.at[c])
        )
    amp_load = pltpu.make_async_copy(amp_hbm, amp, local_s.at[len(starts)])
    int_load = pltpu.make_async_copy(integrals_hbm, integrals, local_s.at[len(starts) + 1])
    for load in loads:
        load.start()
    amp_load.start()

    def mark(u, _):
        shape = (LANES, GROUP * LANES)
        row = lax.broadcasted_iota(jnp.int32, shape, 0)
        col = lax.broadcasted_iota(jnp.int32, shape, 1)
        target = (row // COL) * LANES + u * COL + row % COL
        perm[pl.ds(pl.multiple_of(u * LANES, LANES), LANES), :] = jnp.where(col == target, 1.0, 0.0).astype(BF)
        return 0

    lax.fori_loop(0, GROUP, mark, 0)
    cells[...] = jnp.zeros_like(cells)

    for c, at in enumerate(starts):
        size = min(VROWS, nao - at)
        loads[c].wait()
        for t in range(tiles):
            vf[t, at : at + size, :] = vbuf[at : at + size, t * LANES : (t + 1) * LANES].astype(F32)

    tile0 = sp * COL // LANES
    sub0 = pl.multiple_of((sp * COL) % LANES, COL)

    def pick(b, _):
        to = pl.multiple_of(b * COL, COL)
        for t in range(tiles):
            right[pl.ds(to, COL), t * LANES : (t + 1) * LANES] = vf[t, pl.ds(off[1, b], COL), :].astype(BF)
        lrows[pl.ds(pl.multiple_of(b * ROW, ROW), ROW), :] = vf[tile0, pl.ds(off[0, b], ROW), :]
        return 0

    lax.fori_loop(0, nblk, pick, 0, unroll=2)

    owner = lax.broadcasted_iota(jnp.int32, (nblk, nblk * COL), 1) // COL
    repeat = jnp.where(lax.broadcasted_iota(jnp.int32, (nblk, nblk * COL), 0) == owner, 1.0, 0.0).astype(BF)
    for i in range(ROW):
        lt[i] = lrows[pl.ds(i, nblk, stride=ROW), :].T
        mine = jnp.dot(lt[i, pl.ds(sub0, COL), :].astype(BF), repeat, preferred_element_type=F32)
        spread_e[i * COL : (i + 1) * COL, :] = mine
        for g in range(groups):
            spread_a[g, pl.ds(i, COL, stride=ROW), :] = mine[:, g * LANES : (g + 1) * LANES]

    amp_load.wait()
    int_load.start()
    step = 256
    for n in range(0, nblk * COL, step):
        got = lax.dot_general(
            amp[...], right[n : n + step, :], (((1,), (1,)), ((), ())), preferred_element_type=F32
        )
        got = got.astype(BF).astype(F32)
        for t in range(step // LANES):
            half[n // LANES + t] = got[:, t * LANES : (t + 1) * LANES]

    for g in range(groups):

        lefts = [spread_a[g, a * ROW : (a + 1) * ROW, :] for a in range(COL)]

        def contract(p, _):
            total = lefts[0] * half[g, pl.ds(p * COL, ROW, stride=0), :]
            for a in range(1, COL):
                total = total + lefts[a] * half[g, pl.ds(p * COL + a, ROW, stride=0), :]
            cells[pl.ds(pl.multiple_of(g * PAD * ROW + p * ROW, ROW), ROW), :] = total
            return 0

        lax.fori_loop(0, pairs, contract, 0, unroll=2)
        for i in range(ROW):
            stacked[g * PAD : (g + 1) * PAD, i * LANES : (i + 1) * LANES] = cells[
                pl.ds(g * PAD * ROW + i, PAD, stride=ROW), :
            ].astype(BF)
    moved = jnp.dot(stacked[...], perm[...], preferred_element_type=F32)
    for g in range(groups):
        for v in range(GROUP):
            for j in range(pieces):
                part[v % 2, (g * GROUP + v) // 2, j] = moved[
                    g * PAD + j * SUB : g * PAD + (j + 1) * SUB, v * LANES : (v + 1) * LANES
                ].astype(BF)

    hit = lax.broadcasted_iota(jnp.int32, (COL, next_), 1) == (
        lax.broadcasted_iota(jnp.int32, (COL, next_), 0) + sp * COL
    )
    own_energy = jnp.sum(jnp.where(hit, energies[...], 0.0), axis=1, keepdims=True)

    pl.semaphore_wait(barrier, chips + nz - 1)

    def row_to(t):
        return (y + far_first(t, NY)) % NY

    def row_from(t):
        return (y + NY - far_first(t, NY)) % NY

    def swap(t):
        span = pl.ds(row_to(t) * NX, NX)
        return pltpu.make_async_remote_copy(
            part.at[1 - core, span], pairsum.at[span], pair_s, pair_r.at[t],
            device_id=other, device_id_type=MESH,
        )

    def swap_go(t, _):
        swap(t).start()
        return 0

    def scatter_go(t, _):
        row = row_to(t)
        span = pl.ds(row * NX, NX)
        swap(t).wait_recv()
        outgoing[span] = (part[core, span].astype(F32) + pairsum[span].astype(F32)).astype(BF)
        for u in range(NX):
            to = row * NX + (x + far_first(u, NX)) % NX

            @pl.when(t * NX + u < chips - 1)
            def _():
                pltpu.make_async_remote_copy(
                    outgoing.at[to], arrived.at[chip], rs_s, rs_r,
                    device_id=(to * 2 + core, z), device_id_type=MESH,
                ).start()

        return 0

    lax.fori_loop(0, NY, swap_go, 0)
    lax.fori_loop(0, NY, scatter_go, 0)

    most = pl.ds(0, chips - 1)
    scatter_all = pltpu.make_async_remote_copy(
        outgoing.at[most], arrived.at[most], rs_s, rs_r, device_id=other, device_id_type=MESH
    )

    def diagonal(p, _):
        at = pl.multiple_of(p * COL, COL)
        diag[pl.ds(at, COL), :] = (own_energy + energies[...]) * amp[pl.ds(at, COL), :].astype(F32)
        return 0

    lax.fori_loop(0, pairs, diagonal, 0)
    arrived[chip] = outgoing[chip]
    scatter_all.wait_recv()
    ao_own[...] = lax.fori_loop(
        1, chips, lambda c, total: total + arrived[c].astype(F32), arrived[0].astype(F32), unroll=4
    ).astype(BF)

    def gather(own, landing, send, recv, fsend, frecv):
        def begin(t, _):
            pltpu.make_async_remote_copy(
                own, landing.at[core, chip], send, recv.at[t // NX],
                device_id=(peer(t) * 2 + core, z), device_id_type=MESH,
            ).start()
            return 0

        def row_copy(t, side):
            span = pl.ds(row_from(t) * NX, NX)
            return pltpu.make_async_remote_copy(
                landing.at[side, span], landing.at[side, span], fsend, frecv,
                device_id=other, device_id_type=MESH,
            )

        def come(t, size):
            span = pl.ds(row_from(t) * NX, size)
            return pltpu.make_async_remote_copy(
                landing.at[core, span], landing.at[core, span], send, recv.at[t],
                device_id=other, device_id_type=MESH,
            )

        lax.fori_loop(0, chips - 1, begin, 0)
        landing[core, chip] = own[...]
        come(NY - 1, NX - 1).wait_recv()
        row_copy(NY - 1, core).start()

        def relay(t, _):
            come(NY - 2 - t, NX).wait_recv()
            row_copy(NY - 2 - t, core).start()
            return 0

        lax.fori_loop(0, NY - 1, relay, 0)
        whole = pltpu.make_async_remote_copy(
            landing.at[core], landing.at[1 - core], fsend, frecv, device_id=other, device_id_type=MESH
        )
        whole.wait_recv()

        def drain():
            pltpu.make_async_remote_copy(
                landing.at[core, most], landing.at[core, most], send, recv.at[0],
                device_id=other, device_id_type=MESH,
            ).wait_send()
            whole.wait_send()

        return drain

    drain_ao = gather(ao_own, ao_all, ag_s, ag_r, fw_s, fw_r)

    for k in range(slots):
        b = screened[0, k]
        tile = jnp.where(k < counts[0], ao_all[b % 2, b // 2].astype(F32), 0.0)
        for j in range(pieces):
            chosen[j * SUB : (j + 1) * SUB, k * WIDTH : (k + 1) * WIDTH] = tile[j]
    int_load.wait()
    raw = lax.dot_general(
        chosen[...].astype(BF), integrals[...], (((1,), (1,)), ((), ())), preferred_element_type=F32
    )
    for j in range(pieces):
        raw_own[j] = raw[j * SUB : (j + 1) * SUB, :].astype(BF)

    def along(t, _):
        pltpu.make_async_remote_copy(
            raw_own, raw_all.at[z], z_s, z_r,
            device_id=(sp, (z + far_first(t, nz)) % nz), device_id_type=MESH,
        ).start()
        return 0

    lax.fori_loop(0, nz - 1, along, 0)
    raw_all[z] = raw_own[...]
    rest = pl.ds(0, nz - 1)
    along_all = pltpu.make_async_remote_copy(
        raw_all.at[rest], raw_all.at[rest], z_s, z_r, device_id=other, device_id_type=MESH
    )
    along_all.wait_recv()
    for q in range(nz):
        for j in range(pieces):
            at = q * pairs + j * SUB
            raw_rows[at : at + SUB, :] = raw_all[q, j].astype(F32)
    mix = jnp.dot(coupling[...], raw_rows[...].astype(BF), preferred_element_type=F32)
    for j in range(pieces):
        mix_own[j] = mix[j * SUB : (j + 1) * SUB, :].astype(BF)

    drain_mix = gather(mix_own, mixed_all, mg_s, mg_r, mf_s, mf_r)

    for b in range(nblk):
        block = mixed_all[b % 2, b // 2].astype(F32)
        for j in range(pieces):
            cells[b * PAD + j * SUB : b * PAD + (j + 1) * SUB, :] = block[j]
    for g in range(groups):
        for v in range(GROUP):
            at = (g * GROUP + v) * PAD
            stacked[g * PAD : (g + 1) * PAD, v * LANES : (v + 1) * LANES] = cells[at : at + PAD, :].astype(BF)
    moved = jnp.dot(stacked[...], perm[...], preferred_element_type=F32)
    for i in range(ROW):
        cells[i * groups * PAD : (i + 1) * groups * PAD, :] = moved[:, i * LANES : (i + 1) * LANES]
    for g in range(groups):
        lanes = slice(g * LANES, (g + 1) * LANES)

        lefts = [spread_e[i * COL : (i + 1) * COL, lanes] for i in range(ROW)]

        def lift(p, _):
            total = None
            for i in range(ROW):
                line = cells[pl.ds(i * groups * PAD + g * PAD + p, ROW, stride=0), :]
                term = lefts[i] * jnp.concatenate([line, line], axis=0)
                total = term if total is None else total + term
            upper[pl.ds(pl.multiple_of(p * COL, COL), COL), lanes] = total.astype(BF)
            return 0

        lax.fori_loop(0, pairs, lift, 0, unroll=2)

    step = 256
    for n in range(0, next_, step):
        inner = jnp.dot(upper[...], right[:, n : n + step], preferred_element_type=F32)
        out[:, n : n + step] = (inner + diag[:, n : n + step]).astype(BF)

    pltpu.make_async_remote_copy(
        part.at[1 - core], pairsum, pair_s, pair_r.at[0], device_id=other, device_id_type=MESH
    ).wait_send()
    scatter_all.wait_send()
    drain_ao()
    along_all.wait_send()
    drain_mix()


def residual(offsets, screened, counts, virtuals, amp, integrals, coupling, energies, nz):
    nao, next_ = virtuals.shape
    rows = amp.shape[0]
    pairs = rows // COL
    pieces = pairs // SUB
    nblk = offsets.shape[1]
    groups = nblk // GROUP
    chips = NX * NY
    slots = screened.shape[1]
    vmem = pl.BlockSpec(memory_space=pltpu.VMEM)
    smem = pl.BlockSpec(memory_space=pltpu.SMEM)
    hbm = pl.BlockSpec(memory_space=pltpu.HBM)
    dma = pltpu.SemaphoreType.DMA
    message = (pieces, SUB, WIDTH)
    return pl.pallas_call(
        residual_kernel,
        out_shape=jax.ShapeDtypeStruct((rows, next_), BF),
        in_specs=[smem, smem, smem, hbm, hbm, hbm, vmem, vmem],
        out_specs=vmem,
        scratch_shapes=[
            pltpu.VMEM((nblk * COL, next_), BF),
            pltpu.VMEM((rows, nblk * COL), BF),
            pltpu.VMEM((rows, next_), F32),
            pltpu.VMEM((nao, next_), BF),
            pltpu.VMEM((next_ // LANES, nao, LANES), F32),
            pltpu.VMEM((rows, next_), BF),
            pltpu.VMEM(integrals.shape, BF),
            pltpu.VMEM((GROUP * LANES, GROUP * LANES), BF),
            pltpu.VMEM((groups, rows, LANES), F32),
            pltpu.VMEM((nblk * ROW, LANES), F32),
            pltpu.VMEM((ROW, LANES, nblk), F32),
            pltpu.VMEM((ROW * COL, nblk * COL), F32),
            pltpu.VMEM((groups, COL * ROW, LANES), F32),
            pltpu.VMEM((groups * PAD * ROW, LANES), F32),
            pltpu.VMEM((groups * PAD, ROW * LANES), BF),
            pltpu.VMEM((2, chips, *message), BF),
            pltpu.VMEM((chips, *message), BF),
            pltpu.VMEM((chips, *message), BF),
            pltpu.VMEM((chips, *message), BF),
            pltpu.VMEM(message, BF),
            pltpu.VMEM((2, chips, *message), BF),
            pltpu.VMEM((pairs, slots * WIDTH), F32),
            pltpu.VMEM(message, BF),
            pltpu.VMEM((nz, *message), BF),
            pltpu.VMEM((nz * pairs, WIDTH), F32),
            pltpu.VMEM(message, BF),
            pltpu.VMEM((2, chips, *message), BF),
            dma((-(-nao // VROWS) + 2,)),
            dma, dma((NY,)),
            dma, dma,
            dma, dma((NY,)), dma, dma,
            dma, dma,
            dma, dma((NY,)), dma, dma,
        ],
        compiler_params=pltpu.CompilerParams(
            collective_id=0, has_side_effects=True, vmem_limit_bytes=58 * 1024 * 1024
        ),
        name="residual",
    )(offsets, screened, counts, virtuals, amp, integrals, coupling, energies)


def shards(amplitudes, virtuals, energies, integrals, screened, counts, offsets, coupling):
    pairs, ext, next_ = amplitudes.shape
    amp = amplitudes.reshape(pairs * ext, next_)
    nz = coupling.shape[1] // pairs
    out = residual(offsets, screened, counts, virtuals, amp, integrals, coupling, energies.reshape(1, next_), nz)
    return out.reshape(pairs, ext, next_)


def solution(mesh):
    return jax.shard_map(
        shards,
        mesh=mesh,
        in_specs=(
            P("pb", "sp", None),
            P(),
            P(),
            P("sp", None),
            P("sp", None),
            P("sp"),
            P(),
            P("pb", None),
        ),
        out_specs=P("pb", "sp", None),
        check_vma=False,
    )
```

```python
import functools

import jax
import jax.numpy as jnp
from jax import lax
from jax.experimental import pallas as pl
from jax.experimental.pallas import tpu as pltpu
from jax.sharding import PartitionSpec as P

ROW = 8
COL = 16
WIDTH = ROW * COL
LANES = 128
GROUP = LANES // COL
SUB = 4
BF = jnp.bfloat16
F32 = jnp.float32
MESH = pl.DeviceIdType.MESH
PAD = 24
VROWS = 176
NX, NY = 4, 8
BOTH = 4


def far_first(t, size):
    return size // 2 + (1 - 2 * (t % 2)) * ((t + 1) // 2)


def residual_kernel(
    off, screened, counts, virt, amp_hbm, integrals_hbm, coupling_hbm, energies_hbm, out_hbm,
    right, upper, diag, out, coupling, energies, vbuf, vf, amp, integrals, perm, half, lrows, lt, spread_e, spread_a, cells, stacked,
    part, pairsum, outgoing, arrived, ao_own, ao_all, chosen, raw_own, raw_all, raw_rows, mix_own, mixed_all,
    local_s, pair_s, pair_r, rs_s, rs_r, ag_s, ag_r, fw_s, fw_r, z_s, z_r, mg_s, mg_r, mf_s, mf_r,
):
    nao, next_ = virt.shape
    rows = amp.shape[0]
    pairs = rows // COL
    pieces = pairs // SUB
    nblk = off.shape[1]
    groups = nblk // GROUP
    tiles = next_ // LANES
    slots = screened.shape[1]
    chips = NX * NY

    sp = lax.axis_index("sp")
    z = lax.axis_index("pb")
    nz = lax.axis_size("pb")
    core = sp % 2
    chip = sp // 2
    x = chip % NX
    y = chip // NX
    other = (chip * 2 + (1 - core), z)

    row_list = [lax.rem(y + far_first(t, NY), NY) for t in range(NY)]
    col_list = [lax.rem(x + far_first(u, NX), NX) for u in range(NX)]
    row_chip = [row * NX for row in row_list]
    row_core = [first * 2 + core for first in row_chip]
    col_core = [col * 2 for col in col_list]
    peers = [(t, u) for t in range(NY) for u in range(NX)][:-1]

    def member(t, u):
        return (row_core[t] + col_core[u], z)

    starts = list(range(0, nao, VROWS))
    loads = []
    for c, at in enumerate(starts):
        size = min(VROWS, nao - at)
        loads.append(
            pltpu.make_async_copy(virt.at[pl.ds(at, size)], vbuf.at[pl.ds(at, size)], local_s.at[c])
        )
    amp_load = pltpu.make_async_copy(amp_hbm, amp, local_s.at[len(starts)])
    int_load = pltpu.make_async_copy(integrals_hbm, integrals, local_s.at[len(starts) + 1])
    coupling_load = pltpu.make_async_copy(coupling_hbm, coupling, local_s.at[len(starts) + 2])
    energy_load = pltpu.make_async_copy(energies_hbm, energies, local_s.at[len(starts) + 3])
    for load in loads:
        load.start()
    amp_load.start()

    barrier = pltpu.get_barrier_semaphore()
    for t, u in peers:
        pl.semaphore_signal(barrier, inc=1, device_id=member(t, u), device_id_type=MESH)
    z_list = [lax.rem(z + far_first(t, nz), nz) for t in range(nz)]
    for t in range(nz - 1):
        pl.semaphore_signal(barrier, inc=1, device_id=(sp, z_list[t]), device_id_type=MESH)
    pl.semaphore_signal(barrier, inc=1, device_id=other, device_id_type=MESH)

    def mark(u, _):
        shape = (LANES, GROUP * LANES)
        row = lax.broadcasted_iota(jnp.int32, shape, 0)
        col = lax.broadcasted_iota(jnp.int32, shape, 1)
        target = (row // COL) * LANES + u * COL + row % COL
        perm[pl.ds(pl.multiple_of(u * LANES, LANES), LANES), :] = jnp.where(col == target, 1.0, 0.0).astype(BF)
        return 0

    lax.fori_loop(0, GROUP, mark, 0)
    cells[...] = jnp.zeros_like(cells)

    for c, at in enumerate(starts):
        size = min(VROWS, nao - at)
        loads[c].wait()
        for t in range(tiles):
            vf[t, at : at + size, :] = vbuf[at : at + size, t * LANES : (t + 1) * LANES].astype(F32)

    tile0 = sp * COL // LANES
    sub0 = pl.multiple_of((sp * COL) % LANES, COL)

    for g in range(groups):

        def pick(j, _):
            owner = row_list[g] * GROUP + j
            to = pl.multiple_of(g * LANES + j * COL, COL)
            for t in range(tiles):
                right[pl.ds(to, COL), t * LANES : (t + 1) * LANES] = vf[t, pl.ds(off[1, owner], COL), :].astype(BF)
            at = pl.multiple_of((g * GROUP + j) * ROW, ROW)
            lrows[pl.ds(at, ROW), :] = vf[tile0, pl.ds(off[0, owner], ROW), :]
            return 0

        lax.fori_loop(0, GROUP, pick, 0, unroll=2)

    owner = lax.broadcasted_iota(jnp.int32, (nblk, nblk * COL), 1) // COL
    repeat = jnp.where(lax.broadcasted_iota(jnp.int32, (nblk, nblk * COL), 0) == owner, 1.0, 0.0).astype(BF)
    for i in range(ROW):
        lt[i] = lrows[pl.ds(i, nblk, stride=ROW), :].T
        mine = jnp.dot(lt[i, pl.ds(sub0, COL), :].astype(BF), repeat, preferred_element_type=F32)
        spread_e[i * COL : (i + 1) * COL, :] = mine
        for g in range(groups):
            spread_a[g, pl.ds(i, COL, stride=ROW), :] = mine[:, g * LANES : (g + 1) * LANES]

    amp_load.wait()
    int_load.start()
    coupling_load.start()
    energy_load.start()

    def swap(t):
        span = pl.ds(row_chip[t], NX)
        return pltpu.make_async_remote_copy(
            part.at[1 - core, span], pairsum.at[span], pair_s, pair_r.at[t],
            device_id=other, device_id_type=MESH,
        )

    def scatter(t):
        span = pl.ds(row_chip[t], NX)
        swap(t).wait_recv()
        outgoing[span] = (part[core, span].astype(F32) + pairsum[span].astype(F32)).astype(BF)
        for u in range(NX):
            if (t, u) in peers:
                pltpu.make_async_remote_copy(
                    outgoing.at[row_chip[t] + col_list[u]], arrived.at[chip], rs_s, rs_r,
                    device_id=member(t, u), device_id_type=MESH,
                ).start()

    both = BOTH
    steps = NY // both
    step = both * LANES
    wide = 2 * LANES
    for k in range(steps):
        for n in range(k * step, (k + 1) * step, wide):
            got = lax.dot_general(
                amp[...], right[n : n + wide, :], (((1,), (1,)), ((), ())), preferred_element_type=F32
            )
            got = got.astype(BF).astype(F32)
            for t in range(wide // LANES):
                half[n // LANES + t] = got[:, t * LANES : (t + 1) * LANES]
        for g in range(k * both, (k + 1) * both):
            lefts = [spread_a[g, a * ROW : (a + 1) * ROW, :] for a in range(COL)]

            def contract(p, _):
                total = lefts[0] * half[g, pl.ds(p * COL, ROW, stride=0), :]
                for a in range(1, COL):
                    total = total + lefts[a] * half[g, pl.ds(p * COL + a, ROW, stride=0), :]
                cells[pl.ds(pl.multiple_of(g * PAD * ROW + p * ROW, ROW), ROW), :] = total
                return 0

            lax.fori_loop(0, pairs, contract, 0, unroll=4)
            for i in range(ROW):
                stacked[g * PAD : (g + 1) * PAD, i * LANES : (i + 1) * LANES] = cells[
                    pl.ds(g * PAD * ROW + i, PAD, stride=ROW), :
                ].astype(BF)
        moved = jnp.dot(
            stacked[k * both * PAD : (k + 1) * both * PAD, :], perm[...], preferred_element_type=F32
        )
        for g in range(both):
            for v in range(GROUP):
                for j in range(pieces):
                    part[v % 2, row_chip[k * both + g] + v // 2, j] = moved[
                        g * PAD + j * SUB : g * PAD + (j + 1) * SUB, v * LANES : (v + 1) * LANES
                    ].astype(BF)
        if k == 0:
            pl.semaphore_wait(barrier, chips + nz - 1)
        for t in range(k * both, (k + 1) * both):
            swap(t).start()
        if k > 0:
            for t in range((k - 1) * both, k * both):
                scatter(t)
    for t in range((steps - 1) * both, steps * both):
        scatter(t)

    most = pl.ds(0, chips - 1)
    scatter_all = pltpu.make_async_remote_copy(
        outgoing.at[most], arrived.at[most], rs_s, rs_r, device_id=other, device_id_type=MESH
    )

    energy_load.wait()
    hit = lax.broadcasted_iota(jnp.int32, (COL, next_), 1) == (
        lax.broadcasted_iota(jnp.int32, (COL, next_), 0) + sp * COL
    )
    own_energy = jnp.sum(jnp.where(hit, energies[...], 0.0), axis=1, keepdims=True)

    def diagonal(p, _):
        at = pl.multiple_of(p * COL, COL)
        diag[pl.ds(at, COL), :] = (own_energy + energies[...]) * amp[pl.ds(at, COL), :].astype(F32)
        return 0

    lax.fori_loop(0, pairs, diagonal, 0)
    arrived[chip] = outgoing[chip]
    scatter_all.wait_recv()
    ao_own[...] = lax.fori_loop(
        1, chips, lambda c, total: total + arrived[c].astype(F32), arrived[0].astype(F32), unroll=4
    ).astype(BF)

    def gather(own, landing, send, recv, fsend, frecv):
        def come(t, size):
            span = pl.ds(row_chip[t], size)
            return pltpu.make_async_remote_copy(
                landing.at[core, span], landing.at[core, span], send, recv.at[row_list[t]],
                device_id=other, device_id_type=MESH,
            )

        def forward(t):
            span = pl.ds(row_chip[t], NX)
            return pltpu.make_async_remote_copy(
                landing.at[core, span], landing.at[core, span], fsend, frecv,
                device_id=other, device_id_type=MESH,
            )

        for t, u in peers:
            pltpu.make_async_remote_copy(
                own, landing.at[core, chip], send, recv.at[y],
                device_id=member(t, u), device_id_type=MESH,
            ).start()
        landing[core, chip] = own[...]
        come(NY - 1, NX - 1).wait_recv()
        forward(NY - 1).start()

        for t in reversed(range(NY - 1)):
            come(t, NX).wait_recv()
            forward(t).start()
        whole = pltpu.make_async_remote_copy(
            landing.at[core], landing.at[1 - core], fsend, frecv, device_id=other, device_id_type=MESH
        )
        whole.wait_recv()

        def drain():
            pltpu.make_async_remote_copy(
                landing.at[core, most], landing.at[core, most], send, recv.at[0],
                device_id=other, device_id_type=MESH,
            ).wait_send()
            whole.wait_send()

        return drain

    drain_ao = gather(ao_own, ao_all, ag_s, ag_r, fw_s, fw_r)

    for k in range(slots):
        b = screened[0, k]
        tile = jnp.where(k < counts[0], ao_all[b % 2, b // 2].astype(F32), 0.0)
        for j in range(pieces):
            chosen[j * SUB : (j + 1) * SUB, k * WIDTH : (k + 1) * WIDTH] = tile[j]
    int_load.wait()
    raw = lax.dot_general(
        chosen[...].astype(BF), integrals[...], (((1,), (1,)), ((), ())), preferred_element_type=F32
    )
    for j in range(pieces):
        raw_own[j] = raw[j * SUB : (j + 1) * SUB, :].astype(BF)

    for t in range(nz - 1):
        pltpu.make_async_remote_copy(
            raw_own, raw_all.at[z], z_s, z_r, device_id=(sp, z_list[t]), device_id_type=MESH
        ).start()
    raw_all[z] = raw_own[...]
    rest = pl.ds(0, nz - 1)
    along_all = pltpu.make_async_remote_copy(
        raw_all.at[rest], raw_all.at[rest], z_s, z_r, device_id=other, device_id_type=MESH
    )
    along_all.wait_recv()
    for q in range(nz):
        for j in range(pieces):
            at = q * pairs + j * SUB
            raw_rows[at : at + SUB, :] = raw_all[q, j].astype(F32)
    coupling_load.wait()
    mix = jnp.dot(coupling[...], raw_rows[...].astype(BF), preferred_element_type=F32)
    for j in range(pieces):
        mix_own[j] = mix[j * SUB : (j + 1) * SUB, :].astype(BF)

    drain_mix = gather(mix_own, mixed_all, mg_s, mg_r, mf_s, mf_r)

    for b in range(nblk):
        block = mixed_all[b % 2, row_chip[b // GROUP] + (b % GROUP) // 2].astype(F32)
        for j in range(pieces):
            cells[b * PAD + j * SUB : b * PAD + (j + 1) * SUB, :] = block[j]
    for g in range(groups):
        for v in range(GROUP):
            at = (g * GROUP + v) * PAD
            stacked[g * PAD : (g + 1) * PAD, v * LANES : (v + 1) * LANES] = cells[at : at + PAD, :].astype(BF)
    moved = jnp.dot(stacked[...], perm[...], preferred_element_type=F32)
    for i in range(ROW):
        cells[i * groups * PAD : (i + 1) * groups * PAD, :] = moved[:, i * LANES : (i + 1) * LANES]
    for g in range(groups):
        lanes = slice(g * LANES, (g + 1) * LANES)

        lefts = [spread_e[i * COL : (i + 1) * COL, lanes] for i in range(ROW)]

        def lift(p, _):
            total = None
            for i in range(ROW):
                line = cells[pl.ds(i * groups * PAD + g * PAD + p, ROW, stride=0), :]
                term = lefts[i] * jnp.concatenate([line, line], axis=0)
                total = term if total is None else total + term
            upper[pl.ds(pl.multiple_of(p * COL, COL), COL), lanes] = total.astype(BF)
            return 0

        lax.fori_loop(0, pairs, lift, 0, unroll=2)

    stores = []
    for n in range(0, next_, wide):
        span = slice(n, n + wide)
        total = diag[:, span] + jnp.dot(upper[...], right[:, span], preferred_element_type=F32)
        out[:, span] = total.astype(BF)
        stores.append(
            pltpu.make_async_copy(
                out.at[:, pl.ds(n, wide)], out_hbm.at[:, pl.ds(n, wide)], local_s.at[n // wide]
            )
        )
        stores[-1].start()
    for store in stores:
        store.wait()

    pltpu.make_async_remote_copy(
        part.at[1 - core], pairsum, pair_s, pair_r.at[0], device_id=other, device_id_type=MESH
    ).wait_send()
    scatter_all.wait_send()
    drain_ao()
    along_all.wait_send()
    drain_mix()


def residual(offsets, screened, counts, virtuals, amp, integrals, coupling, energies, nz):
    nao, next_ = virtuals.shape
    rows = amp.shape[0]
    pairs = rows // COL
    pieces = pairs // SUB
    nblk = offsets.shape[1]
    groups = nblk // GROUP
    chips = NX * NY
    slots = screened.shape[1]
    smem = pl.BlockSpec(memory_space=pltpu.SMEM)
    hbm = pl.BlockSpec(memory_space=pltpu.HBM)
    dma = pltpu.SemaphoreType.DMA
    message = (pieces, SUB, WIDTH)
    return pl.pallas_call(
        residual_kernel,
        out_shape=jax.ShapeDtypeStruct((rows, next_), BF),
        in_specs=[smem, smem, smem, hbm, hbm, hbm, hbm, hbm],
        out_specs=hbm,
        scratch_shapes=[
            pltpu.VMEM((nblk * COL, next_), BF),
            pltpu.VMEM((rows, nblk * COL), BF),
            pltpu.VMEM((rows, next_), F32),
            pltpu.VMEM((rows, next_), BF),
            pltpu.VMEM(coupling.shape, BF),
            pltpu.VMEM(energies.shape, F32),
            pltpu.VMEM((nao, next_), BF),
            pltpu.VMEM((next_ // LANES, nao, LANES), F32),
            pltpu.VMEM((rows, next_), BF),
            pltpu.VMEM(integrals.shape, BF),
            pltpu.VMEM((GROUP * LANES, GROUP * LANES), BF),
            pltpu.VMEM((groups, rows, LANES), F32),
            pltpu.VMEM((nblk * ROW, LANES), F32),
            pltpu.VMEM((ROW, LANES, nblk), F32),
            pltpu.VMEM((ROW * COL, nblk * COL), F32),
            pltpu.VMEM((groups, COL * ROW, LANES), F32),
            pltpu.VMEM((groups * PAD * ROW, LANES), F32),
            pltpu.VMEM((groups * PAD, ROW * LANES), BF),
            pltpu.VMEM((2, chips, *message), BF),
            pltpu.VMEM((chips, *message), BF),
            pltpu.VMEM((chips, *message), BF),
            pltpu.VMEM((chips, *message), BF),
            pltpu.VMEM(message, BF),
            pltpu.VMEM((2, chips, *message), BF),
            pltpu.VMEM((pairs, slots * WIDTH), F32),
            pltpu.VMEM(message, BF),
            pltpu.VMEM((nz, *message), BF),
            pltpu.VMEM((nz * pairs, WIDTH), F32),
            pltpu.VMEM(message, BF),
            pltpu.VMEM((2, chips, *message), BF),
            dma((-(-nao // VROWS) + 4,)),
            dma, dma((NY,)),
            dma, dma,
            dma, dma((NY,)), dma, dma,
            dma, dma,
            dma, dma((NY,)), dma, dma,
        ],
        compiler_params=pltpu.CompilerParams(
            collective_id=0, has_side_effects=True, vmem_limit_bytes=58 * 1024 * 1024
        ),
        name="residual",
    )(offsets, screened, counts, virtuals, amp, integrals, coupling, energies)


def shards(amplitudes, virtuals, energies, integrals, screened, counts, offsets, coupling):
    pairs, ext, next_ = amplitudes.shape
    amp = amplitudes.reshape(pairs * ext, next_)
    nz = coupling.shape[1] // pairs
    out = residual(offsets, screened, counts, virtuals, amp, integrals, coupling, energies.reshape(1, next_), nz)
    return out.reshape(pairs, ext, next_)


def solution(mesh):
    return jax.shard_map(
        shards,
        mesh=mesh,
        in_specs=(
            P("pb", "sp", None),
            P(),
            P(),
            P("sp", None),
            P("sp", None),
            P("sp"),
            P(),
            P("pb", None),
        ),
        out_specs=P("pb", "sp", None),
        check_vma=False,
    )
```

```python
import functools

import jax
import jax.numpy as jnp
from jax import lax
from jax.experimental import pallas as pl
from jax.experimental.pallas import tpu as pltpu
from jax.sharding import PartitionSpec as P

ROW = 8
COL = 16
WIDTH = ROW * COL
LANES = 128
GROUP = LANES // COL
SUB = 4
BF = jnp.bfloat16
F32 = jnp.float32
MESH = pl.DeviceIdType.MESH
PAD = 24
VROWS = 176
NX, NY = 4, 8
BOTH = 4


def far_first(t, size):
    return size // 2 + (1 - 2 * (t % 2)) * ((t + 1) // 2)


def residual_kernel(
    off, screened, counts, virt, amp_hbm, integrals_hbm, coupling_hbm, energies_hbm, out_hbm,
    right, upper, diag, out, coupling, energies, vbuf, vf, amp, integrals, perm, half, lrows, lt, spread_e, spread_a, cells, stacked,
    part, pairsum, outgoing, arrived, ao_own, ao_all, chosen, raw_own, raw_all, raw_rows, mix_own, mixed_all,
    local_s, pair_s, pair_r, rs_s, rs_r, ag_s, ag_r, fw_s, fw_r, z_s, z_r, mg_s, mg_r, mf_s, mf_r,
):
    nao, next_ = virt.shape
    rows = amp.shape[0]
    pairs = rows // COL
    pieces = pairs // SUB
    nblk = off.shape[1]
    groups = nblk // GROUP
    tiles = next_ // LANES
    slots = screened.shape[1]
    chips = NX * NY

    sp = lax.axis_index("sp")
    z = lax.axis_index("pb")
    nz = lax.axis_size("pb")
    core = sp % 2
    chip = sp // 2
    x = chip % NX
    y = chip // NX
    other = (chip * 2 + (1 - core), z)

    row_list = [lax.rem(y + far_first(t, NY), NY) for t in range(NY)]
    col_list = [lax.rem(x + far_first(u, NX), NX) for u in range(NX)]
    row_chip = [row * NX for row in row_list]
    row_core = [first * 2 + core for first in row_chip]
    col_core = [col * 2 for col in col_list]
    peers = [(t, u) for t in range(NY) for u in range(NX)][:-1]

    def hops(pair):
        dy, dx = far_first(pair[0], NY), far_first(pair[1], NX)
        return min(dy, NY - dy) + min(dx, NX - dx)

    by_hops = sorted(peers, key=lambda pair: -hops(pair))

    def member(t, u):
        return (row_core[t] + col_core[u], z)

    starts = list(range(0, nao, VROWS))
    loads = []
    for c, at in enumerate(starts):
        size = min(VROWS, nao - at)
        loads.append(
            pltpu.make_async_copy(virt.at[pl.ds(at, size)], vbuf.at[pl.ds(at, size)], local_s.at[c])
        )
    amp_load = pltpu.make_async_copy(amp_hbm, amp, local_s.at[len(starts)])
    int_load = pltpu.make_async_copy(integrals_hbm, integrals, local_s.at[len(starts) + 1])
    coupling_load = pltpu.make_async_copy(coupling_hbm, coupling, local_s.at[len(starts) + 2])
    energy_load = pltpu.make_async_copy(energies_hbm, energies, local_s.at[len(starts) + 3])
    for load in loads:
        load.start()
    amp_load.start()

    barrier = pltpu.get_barrier_semaphore()
    for t, u in peers:
        pl.semaphore_signal(barrier, inc=1, device_id=member(t, u), device_id_type=MESH)
    z_list = [lax.rem(z + far_first(t, nz), nz) for t in range(nz)]
    for t in range(nz - 1):
        pl.semaphore_signal(barrier, inc=1, device_id=(sp, z_list[t]), device_id_type=MESH)
    pl.semaphore_signal(barrier, inc=1, device_id=other, device_id_type=MESH)

    def mark(u, _):
        shape = (LANES, GROUP * LANES)
        row = lax.broadcasted_iota(jnp.int32, shape, 0)
        col = lax.broadcasted_iota(jnp.int32, shape, 1)
        target = (row // COL) * LANES + u * COL + row % COL
        perm[pl.ds(pl.multiple_of(u * LANES, LANES), LANES), :] = jnp.where(col == target, 1.0, 0.0).astype(BF)
        return 0

    lax.fori_loop(0, GROUP, mark, 0)
    cells[...] = jnp.zeros_like(cells)

    for c, at in enumerate(starts):
        size = min(VROWS, nao - at)
        loads[c].wait()
        for t in range(tiles):
            vf[t, at : at + size, :] = vbuf[at : at + size, t * LANES : (t + 1) * LANES].astype(F32)

    tile0 = sp * COL // LANES
    sub0 = pl.multiple_of((sp * COL) % LANES, COL)

    for g in range(groups):

        def pick(j, _):
            owner = row_list[g] * GROUP + j
            to = pl.multiple_of(g * LANES + j * COL, COL)
            for t in range(tiles):
                right[pl.ds(to, COL), t * LANES : (t + 1) * LANES] = vf[t, pl.ds(off[1, owner], COL), :].astype(BF)
            at = pl.multiple_of((g * GROUP + j) * ROW, ROW)
            lrows[pl.ds(at, ROW), :] = vf[tile0, pl.ds(off[0, owner], ROW), :]
            return 0

        lax.fori_loop(0, GROUP, pick, 0, unroll=4)

    owner = lax.broadcasted_iota(jnp.int32, (nblk, nblk * COL), 1) // COL
    repeat = jnp.where(lax.broadcasted_iota(jnp.int32, (nblk, nblk * COL), 0) == owner, 1.0, 0.0).astype(BF)
    for i in range(ROW):
        lt[i] = lrows[pl.ds(i, nblk, stride=ROW), :].T
        mine = jnp.dot(lt[i, pl.ds(sub0, COL), :].astype(BF), repeat, preferred_element_type=F32)
        spread_e[i * COL : (i + 1) * COL, :] = mine
        for g in range(groups):
            spread_a[g, pl.ds(i, COL, stride=ROW), :] = mine[:, g * LANES : (g + 1) * LANES]

    amp_load.wait()
    int_load.start()
    coupling_load.start()
    energy_load.start()

    def swap(t):
        span = pl.ds(row_chip[t], NX)
        return pltpu.make_async_remote_copy(
            part.at[1 - core, span], pairsum.at[span], pair_s, pair_r.at[t],
            device_id=other, device_id_type=MESH,
        )

    def scatter(t):
        span = pl.ds(row_chip[t], NX)
        swap(t).wait_recv()
        outgoing[span] = (part[core, span].astype(F32) + pairsum[span].astype(F32)).astype(BF)
        for u in range(NX):
            if (t, u) in peers:
                pltpu.make_async_remote_copy(
                    outgoing.at[row_chip[t] + col_list[u]], arrived.at[chip], rs_s, rs_r,
                    device_id=member(t, u), device_id_type=MESH,
                ).start()

    both = BOTH
    steps = NY // both
    step = both * LANES
    wide = 2 * LANES
    for k in range(steps):
        for n in range(k * step, (k + 1) * step, wide):
            got = lax.dot_general(
                amp[...], right[n : n + wide, :], (((1,), (1,)), ((), ())), preferred_element_type=F32
            )
            got = got.astype(BF).astype(F32)
            for t in range(wide // LANES):
                half[n // LANES + t] = got[:, t * LANES : (t + 1) * LANES]
        for g in range(k * both, (k + 1) * both):
            lefts = [spread_a[g, a * ROW : (a + 1) * ROW, :] for a in range(COL)]

            def contract(p, _):
                total = lefts[0] * half[g, pl.ds(p * COL, ROW, stride=0), :]
                for a in range(1, COL):
                    total = total + lefts[a] * half[g, pl.ds(p * COL + a, ROW, stride=0), :]
                cells[pl.ds(pl.multiple_of(g * PAD * ROW + p * ROW, ROW), ROW), :] = total
                return 0

            lax.fori_loop(0, pairs, contract, 0, unroll=4)
            for i in range(ROW):
                stacked[g * PAD : (g + 1) * PAD, i * LANES : (i + 1) * LANES] = cells[
                    pl.ds(g * PAD * ROW + i, PAD, stride=ROW), :
                ].astype(BF)
        moved = jnp.dot(
            stacked[k * both * PAD : (k + 1) * both * PAD, :], perm[...], preferred_element_type=F32
        )
        for g in range(both):
            for v in range(GROUP):
                for j in range(pieces):
                    part[v % 2, row_chip[k * both + g] + v // 2, j] = moved[
                        g * PAD + j * SUB : g * PAD + (j + 1) * SUB, v * LANES : (v + 1) * LANES
                    ].astype(BF)
        if k == 0:
            pl.semaphore_wait(barrier, chips + nz - 1)
        for t in range(k * both, (k + 1) * both):
            swap(t).start()
        if k > 0:
            for t in range((k - 1) * both, k * both):
                scatter(t)
    for t in range((steps - 1) * both, steps * both):
        scatter(t)

    most = pl.ds(0, chips - 1)
    scatter_all = pltpu.make_async_remote_copy(
        outgoing.at[most], arrived.at[most], rs_s, rs_r, device_id=other, device_id_type=MESH
    )

    energy_load.wait()
    hit = lax.broadcasted_iota(jnp.int32, (COL, next_), 1) == (
        lax.broadcasted_iota(jnp.int32, (COL, next_), 0) + sp * COL
    )
    own_energy = jnp.sum(jnp.where(hit, energies[...], 0.0), axis=1, keepdims=True)

    def diagonal(p, _):
        at = pl.multiple_of(p * COL, COL)
        diag[pl.ds(at, COL), :] = (own_energy + energies[...]) * amp[pl.ds(at, COL), :].astype(F32)
        return 0

    lax.fori_loop(0, pairs, diagonal, 0)
    arrived[chip] = outgoing[chip]
    scatter_all.wait_recv()
    ao_own[...] = lax.fori_loop(
        1, chips, lambda c, total: total + arrived[c].astype(F32), arrived[0].astype(F32), unroll=4
    ).astype(BF)

    def gather(own, landing, send, recv, fsend, frecv):
        def come(t, size):
            span = pl.ds(row_chip[t], size)
            return pltpu.make_async_remote_copy(
                landing.at[core, span], landing.at[core, span], send, recv.at[row_list[t]],
                device_id=other, device_id_type=MESH,
            )

        def forward(t):
            span = pl.ds(row_chip[t], NX)
            return pltpu.make_async_remote_copy(
                landing.at[core, span], landing.at[core, span], fsend, frecv,
                device_id=other, device_id_type=MESH,
            )

        for t, u in by_hops:
            pltpu.make_async_remote_copy(
                own, landing.at[core, chip], send, recv.at[y],
                device_id=member(t, u), device_id_type=MESH,
            ).start()
        landing[core, chip] = own[...]
        come(NY - 1, NX - 1).wait_recv()
        forward(NY - 1).start()

        for t in reversed(range(NY - 1)):
            come(t, NX).wait_recv()
            forward(t).start()
        whole = pltpu.make_async_remote_copy(
            landing.at[core], landing.at[1 - core], fsend, frecv, device_id=other, device_id_type=MESH
        )
        whole.wait_recv()

        def drain():
            pltpu.make_async_remote_copy(
                landing.at[core, most], landing.at[core, most], send, recv.at[0],
                device_id=other, device_id_type=MESH,
            ).wait_send()
            whole.wait_send()

        return drain

    drain_ao = gather(ao_own, ao_all, ag_s, ag_r, fw_s, fw_r)

    for k in range(slots):
        b = screened[0, k]
        tile = jnp.where(k < counts[0], ao_all[b % 2, b // 2].astype(F32), 0.0)
        for j in range(pieces):
            chosen[j * SUB : (j + 1) * SUB, k * WIDTH : (k + 1) * WIDTH] = tile[j]
    int_load.wait()
    raw = lax.dot_general(
        chosen[...].astype(BF), integrals[...], (((1,), (1,)), ((), ())), preferred_element_type=F32
    )
    for j in range(pieces):
        raw_own[j] = raw[j * SUB : (j + 1) * SUB, :].astype(BF)

    for t in range(nz - 1):
        pltpu.make_async_remote_copy(
            raw_own, raw_all.at[z], z_s, z_r, device_id=(sp, z_list[t]), device_id_type=MESH
        ).start()
    raw_all[z] = raw_own[...]
    rest = pl.ds(0, nz - 1)
    along_all = pltpu.make_async_remote_copy(
        raw_all.at[rest], raw_all.at[rest], z_s, z_r, device_id=other, device_id_type=MESH
    )
    along_all.wait_recv()
    for q in range(nz):
        for j in range(pieces):
            at = q * pairs + j * SUB
            raw_rows[at : at + SUB, :] = raw_all[q, j].astype(F32)
    coupling_load.wait()
    mix = jnp.dot(coupling[...], raw_rows[...].astype(BF), preferred_element_type=F32)
    for j in range(pieces):
        mix_own[j] = mix[j * SUB : (j + 1) * SUB, :].astype(BF)

    drain_mix = gather(mix_own, mixed_all, mg_s, mg_r, mf_s, mf_r)

    for b in range(nblk):
        block = mixed_all[b % 2, row_chip[b // GROUP] + (b % GROUP) // 2].astype(F32)
        for j in range(pieces):
            cells[b * PAD + j * SUB : b * PAD + (j + 1) * SUB, :] = block[j]
    for g in range(groups):
        for v in range(GROUP):
            at = (g * GROUP + v) * PAD
            stacked[g * PAD : (g + 1) * PAD, v * LANES : (v + 1) * LANES] = cells[at : at + PAD, :].astype(BF)
    moved = jnp.dot(stacked[...], perm[...], preferred_element_type=F32)
    for i in range(ROW):
        cells[i * groups * PAD : (i + 1) * groups * PAD, :] = moved[:, i * LANES : (i + 1) * LANES]
    for g in range(groups):
        lanes = slice(g * LANES, (g + 1) * LANES)

        lefts = [spread_e[i * COL : (i + 1) * COL, lanes] for i in range(ROW)]

        def lift(p, _):
            total = None
            for i in range(ROW):
                line = cells[pl.ds(i * groups * PAD + g * PAD + p, ROW, stride=0), :]
                term = lefts[i] * jnp.concatenate([line, line], axis=0)
                total = term if total is None else total + term
            upper[pl.ds(pl.multiple_of(p * COL, COL), COL), lanes] = total.astype(BF)
            return 0

        lax.fori_loop(0, pairs, lift, 0, unroll=4)

    stores = []
    for n in range(0, next_, wide):
        span = slice(n, n + wide)
        total = diag[:, span] + jnp.dot(upper[...], right[:, span], preferred_element_type=F32)
        out[:, span] = total.astype(BF)
        stores.append(
            pltpu.make_async_copy(
                out.at[:, pl.ds(n, wide)], out_hbm.at[:, pl.ds(n, wide)], local_s.at[n // wide]
            )
        )
        stores[-1].start()
    for store in stores:
        store.wait()

    pltpu.make_async_remote_copy(
        part.at[1 - core], pairsum, pair_s, pair_r.at[0], device_id=other, device_id_type=MESH
    ).wait_send()
    scatter_all.wait_send()
    drain_ao()
    along_all.wait_send()
    drain_mix()


def residual(offsets, screened, counts, virtuals, amp, integrals, coupling, energies, nz):
    nao, next_ = virtuals.shape
    rows = amp.shape[0]
    pairs = rows // COL
    pieces = pairs // SUB
    nblk = offsets.shape[1]
    groups = nblk // GROUP
    chips = NX * NY
    slots = screened.shape[1]
    smem = pl.BlockSpec(memory_space=pltpu.SMEM)
    hbm = pl.BlockSpec(memory_space=pltpu.HBM)
    dma = pltpu.SemaphoreType.DMA
    message = (pieces, SUB, WIDTH)
    return pl.pallas_call(
        residual_kernel,
        out_shape=jax.ShapeDtypeStruct((rows, next_), BF),
        in_specs=[smem, smem, smem, hbm, hbm, hbm, hbm, hbm],
        out_specs=hbm,
        scratch_shapes=[
            pltpu.VMEM((nblk * COL, next_), BF),
            pltpu.VMEM((rows, nblk * COL), BF),
            pltpu.VMEM((rows, next_), F32),
            pltpu.VMEM((rows, next_), BF),
            pltpu.VMEM(coupling.shape, BF),
            pltpu.VMEM(energies.shape, F32),
            pltpu.VMEM((nao, next_), BF),
            pltpu.VMEM((next_ // LANES, nao, LANES), F32),
            pltpu.VMEM((rows, next_), BF),
            pltpu.VMEM(integrals.shape, BF),
            pltpu.VMEM((GROUP * LANES, GROUP * LANES), BF),
            pltpu.VMEM((groups, rows, LANES), F32),
            pltpu.VMEM((nblk * ROW, LANES), F32),
            pltpu.VMEM((ROW, LANES, nblk), F32),
            pltpu.VMEM((ROW * COL, nblk * COL), F32),
            pltpu.VMEM((groups, COL * ROW, LANES), F32),
            pltpu.VMEM((groups * PAD * ROW, LANES), F32),
            pltpu.VMEM((groups * PAD, ROW * LANES), BF),
            pltpu.VMEM((2, chips, *message), BF),
            pltpu.VMEM((chips, *message), BF),
            pltpu.VMEM((chips, *message), BF),
            pltpu.VMEM((chips, *message), BF),
            pltpu.VMEM(message, BF),
            pltpu.VMEM((2, chips, *message), BF),
            pltpu.VMEM((pairs, slots * WIDTH), F32),
            pltpu.VMEM(message, BF),
            pltpu.VMEM((nz, *message), BF),
            pltpu.VMEM((nz * pairs, WIDTH), F32),
            pltpu.VMEM(message, BF),
            pltpu.VMEM((2, chips, *message), BF),
            dma((-(-nao // VROWS) + 4,)),
            dma, dma((NY,)),
            dma, dma,
            dma, dma((NY,)), dma, dma,
            dma, dma,
            dma, dma((NY,)), dma, dma,
        ],
        compiler_params=pltpu.CompilerParams(
            collective_id=0, has_side_effects=True, vmem_limit_bytes=58 * 1024 * 1024
        ),
        name="residual",
    )(offsets, screened, counts, virtuals, amp, integrals, coupling, energies)


def shards(amplitudes, virtuals, energies, integrals, screened, counts, offsets, coupling):
    pairs, ext, next_ = amplitudes.shape
    amp = amplitudes.reshape(pairs * ext, next_)
    nz = coupling.shape[1] // pairs
    out = residual(offsets, screened, counts, virtuals, amp, integrals, coupling, energies.reshape(1, next_), nz)
    return out.reshape(pairs, ext, next_)


def solution(mesh):
    return jax.shard_map(
        shards,
        mesh=mesh,
        in_specs=(
            P("pb", "sp", None),
            P(),
            P(),
            P("sp", None),
            P("sp", None),
            P("sp"),
            P(),
            P("pb", None),
        ),
        out_specs=P("pb", "sp", None),
        check_vma=False,
    )
```
